32 devices in a mesh: section: 1, srv: 16 (over z, x, core), tp: 2 (over y).
Axes of the slice: x: 2, y: 2, z: 4, core: 2. Of those that a mesh axis runs over, the one named last changes fastest.
Arguments:
- queries: bfloat16 [2048, 4096], P(('section', 'srv'), 'tp'), may hold values from -40 to 40
- keys: bfloat16 [2048, 512], P(('section', 'srv'), 'tp'), may hold values from -40 to 40
- values: bfloat16 [2048, 512], P(('section', 'srv'), 'tp'), may hold values from -6 to 6
- residual: bfloat16 [2048, 4096], P(('section', 'srv'), 'tp'), may hold values from -6 to 6
- out_weight: bfloat16 [4096, 4096], P('tp', ('section', 'srv')), may hold values from -0.1875 to 0.1875
- norm_gain: float32 [4096], P('tp'), may hold values from 0.25 to 1.75
- level_shift: float32 [8, 4096], P(None, 'tp'), may hold values from -3 to 3
- doc_lengths: int32 [1, 4], P('section'), may hold values from 1 to 64, 128 in all within a row
- noise_level: int32 [1, 4], P('section'), may hold values from 0 to 7
Outputs:
- normed: bfloat16 [2048, 4096], P(('section', 'srv'), 'tp')
The draws below stay inside these ranges and needn't reach their ends.
Inputs may be any that keep to these rules, and one draw needn't show every extreme that they name: `doc_lengths`: each micro-batch's lengths sum to 128.
All inputs are finite; a program needn't handle non-finite values.
Results may differ from the reference program's by a relative error of at most 0.013.
Values may be sent and summed in bfloat16 or wider, within the bound.
No kernel may reach another device: no remote copies, remote signals or barrier semaphores. Data moves between devices by JAX's collectives and lax.ppermute only.
A program may use at most 64 MiB of HBM per device.

```python
import math
import jax
import jax.numpy as jnp
import numpy as np
from jax import lax

D = 4096
QUERY_HEADS = 32
KEY_VALUE_HEADS = 4
HEAD_SIZE = 128
BLK = 16
DOCS = 4
LEVELS = 8
MICRO_BATCH_ROWS = 2048
TOTAL_ROWS = 2048
NBLK = 128
N_SECTION = 1


def random_base_keys(key):
    drawn_samples = jax.random.normal(jax.random.fold_in(key, 11), (TOTAL_ROWS, KEY_VALUE_HEADS * HEAD_SIZE), jnp.float32)
    return drawn_samples


def draw_keys(key, part):
    return random_base_keys(key).astype(jnp.bfloat16)


def draw_queries(key, part):
    drawn_samples = jax.random.normal(jax.random.fold_in(key, 12), (TOTAL_ROWS, QUERY_HEADS * HEAD_SIZE), jnp.float32)
    return drawn_samples.astype(jnp.bfloat16)


def plant(drawn, rng, low, high):
    longest = drawn.shape.index(max(drawn.shape))
    spots = []
    for shift in (0, 1):
        where = [jax.random.randint(jax.random.fold_in(rng, axis), (), 0, length) for axis, length in enumerate(drawn.shape)]
        where[longest] = (where[longest] + shift) % drawn.shape[longest]
        spots.append(tuple(where))
    return drawn.at[spots[0]].set(low).at[spots[1]].set(high)


def steps_of(rng, extent, cuts, smallest, high):
    factor_of, own = 1.0, jax.random.fold_in(rng, 6)
    for dim, blocks in cuts:
        draws = jnp.exp(jax.random.uniform(jax.random.fold_in(own, dim), (blocks,), jnp.float32, smallest / len(cuts), high / len(cuts)))
        factor_of = factor_of * jnp.repeat(draws, extent[dim] // blocks).reshape([-1 if axis == dim else 1 for axis in range(len(extent))])
    return factor_of


def split_up(count, total, reach, lean):
    weights = [(1 << 20) // math.isqrt(rank ** lean) + 1 for rank in range(2, count + 1)]
    spare, holding = total - reach - (count - 1), [1] * (count - 1)
    while spare > 0:
        free = [i for i in range(count - 1) if holding[i] < reach]
        whole, left = sum([weights[i] for i in free]), spare
        for i in free:
            addition = min(reach - holding[i], max(1, left * weights[i] // whole), spare)
            holding[i] = holding[i] + addition
            spare = spare - addition
    return np.array([reach] + holding)


def uneven(key, count, total, reach, skew):
    if count == 2:
        one = jax.random.randint(key, (), max(1, total - reach), min(reach, total - 1) + 1)
        return jnp.stack([one, total - one])
    tallies = jnp.asarray(split_up(count, total, reach, skew), jnp.int32)
    pairs = (count - 1) // 2
    source_of, taker = tallies[1:1 + 2 * pairs:2], tallies[2:2 + 2 * pairs:2]
    margin = jnp.minimum(source_of - 1, reach - taker)
    passed = jax.random.randint(jax.random.fold_in(key, 1), (pairs,), 0, 1 << 20) % (margin + 1)
    tallies = tallies.at[1:1 + 2 * pairs:2].set(source_of - passed).at[2:2 + 2 * pairs:2].set(taker + passed)
    return tallies[jax.random.permutation(jax.random.fold_in(key, 2), count)]


def centred(rng, extent, scale, most, cuts=(), kind=jnp.bfloat16):
    values = scale * jax.random.normal(rng, extent, jnp.float32)
    if cuts:
        values = values * steps_of(rng, extent, cuts, -0.22, 0.18)
    return jnp.clip(values, -most, most).astype(kind)


def setup_inputs(seed: int = 0) -> dict:
    splits = jax.random.split(jax.random.key(seed), 10)
    return {
        "queries": draw_queries(jax.random.fold_in(splits[9], 71), 0),
        "keys": draw_keys(jax.random.fold_in(splits[9], 71), 0),
        "values": centred(splits[2], (TOTAL_ROWS, KEY_VALUE_HEADS * HEAD_SIZE), 1.0, 6.0, ((0, 16), (1, 2))),
        "residual": centred(splits[3], (TOTAL_ROWS, D), 1.0, 6.0, ((0, 16), (1, 2))),
        "out_weight": centred(splits[4], (QUERY_HEADS * HEAD_SIZE, D), (QUERY_HEADS * HEAD_SIZE // 4) ** -0.5, 0.1875, ((0, 2), (1, 16))),
        "norm_gain": jnp.clip(1.0 + 0.15 * jax.random.normal(splits[5], (D,), jnp.float32), 0.25, 1.75),
        "level_shift": centred(splits[6], (LEVELS, D), 0.5, 3.0, ((1, 2),), jnp.float32),
        "doc_lengths": jax.vmap(lambda own: uneven(own, DOCS, NBLK, NBLK // 2, 2))(jax.random.split(splits[7], N_SECTION)).reshape((N_SECTION, DOCS)).astype(jnp.int32),
        "noise_level": plant(jax.random.randint(splits[8], (N_SECTION, DOCS), 0, LEVELS), jax.random.fold_in(splits[8], 1), 0, LEVELS - 1).astype(jnp.int32),
    }


def layout(lengths_blocks):
    lengths = lengths_blocks * BLK
    ends = jnp.cumsum(lengths).astype(jnp.int32)
    starts = (ends - lengths).astype(jnp.int32)
    positions = jnp.arange(MICRO_BATCH_ROWS, dtype=jnp.int32)
    member = (positions[:, None] >= starts[None, :]) & (positions[:, None] < ends[None, :])
    first = lax.optimization_barrier(jnp.sum(jnp.where(member, starts[None, :], 0), axis=1)).astype(jnp.int32)
    limit = (positions // BLK + 1) * BLK
    return (member, first, limit.astype(jnp.int32))

def attend(queries, keys, values, first, limit):
    query_groups = QUERY_HEADS // KEY_VALUE_HEADS
    current_block = 512
    scale = HEAD_SIZE ** (-0.5)
    gathered_keys = keys.astype(jnp.float32).reshape(MICRO_BATCH_ROWS, KEY_VALUE_HEADS, HEAD_SIZE)
    gathered_values = values.astype(jnp.float32).reshape(MICRO_BATCH_ROWS, KEY_VALUE_HEADS, HEAD_SIZE)
    columns = jnp.arange(MICRO_BATCH_ROWS, dtype=jnp.int32)

    def one_block(index):
        begin = (index * current_block).astype(jnp.int32)
        query_rows = lax.dynamic_slice_in_dim(queries, begin, current_block, 0).astype(jnp.float32)
        query_rows = query_rows.reshape(current_block, KEY_VALUE_HEADS, query_groups, HEAD_SIZE)
        lower = lax.dynamic_slice_in_dim(first, begin, current_block, 0)
        upper = lax.dynamic_slice_in_dim(limit, begin, current_block, 0)
        mask = (columns[None, :] >= lower[:, None]) & (columns[None, :] < upper[:, None])
        outputs = []
        for head_number in range(KEY_VALUE_HEADS):
            scores = jnp.einsum('rgd,jd->grj', query_rows[:, head_number], gathered_keys[:, head_number]) * scale
            scores = jnp.where(mask[None], scores, -1e+30)
            best = lax.optimization_barrier(jnp.max(scores, axis=-1, keepdims=True))
            weights = jnp.where(mask[None], jnp.exp(scores - best), 0.0)
            total = lax.optimization_barrier(jnp.sum(weights, axis=-1))
            rounded = weights.astype(jnp.bfloat16).astype(jnp.float32)
            summed = jnp.einsum('grj,jd->grd', rounded, gathered_values[:, head_number])
            outputs.append(summed / total[..., None])
        stacked = jnp.stack(outputs, axis=0)
        return stacked.transpose(2, 0, 1, 3).reshape(current_block, QUERY_HEADS * HEAD_SIZE).astype(jnp.bfloat16)
    pieces = lax.map(one_block, jnp.arange(MICRO_BATCH_ROWS // current_block, dtype=jnp.int32))
    return pieces.reshape(MICRO_BATCH_ROWS, QUERY_HEADS * HEAD_SIZE)

def reference(queries, keys, values, residual, out_weight, norm_gain, level_shift, doc_lengths, noise_level):
    results = []
    for section_index in range(N_SECTION):
        lo = section_index * MICRO_BATCH_ROWS
        hi = lo + MICRO_BATCH_ROWS
        member, first, limit = layout(doc_lengths[section_index])
        attended = attend(queries[lo:hi], keys[lo:hi], values[lo:hi], first, limit)
        hidden = residual[lo:hi].astype(jnp.float32) + jnp.dot(attended, out_weight, preferred_element_type=jnp.float32)
        squares = lax.optimization_barrier(jnp.mean(hidden * hidden, axis=1))
        level = lax.optimization_barrier(jnp.sum(jnp.where(member, noise_level[section_index][None, :], 0), axis=1)).astype(jnp.int32)
        onehot = (level[:, None] == jnp.arange(LEVELS, dtype=jnp.int32)[None, :]).astype(jnp.float32)
        shift = jnp.dot(onehot, level_shift, precision=lax.Precision.HIGHEST)
        normed = hidden * lax.rsqrt(squares + 1e-06)[:, None] * norm_gain[None, :] * (1.0 + shift)
        results.append(normed.astype(jnp.bfloat16))
    return jnp.concatenate(results, axis=0)
```

```python
import functools
import jax
import jax.numpy as jnp
from jax import lax
from jax.experimental import pallas as pl
from jax.experimental.pallas import tpu as pltpu
from jax.sharding import PartitionSpec as P

HEAD_SIZE = 128
BLK = 16
LOW_BITS = 2


def flipped(block, mask, axis="srv"):
    devices = range(lax.axis_size(axis))
    return lax.ppermute(block, axis, [(i, i ^ mask) for i in devices])


def shifted(block, axis, distance):
    devices = range(lax.axis_size(axis))
    route = [(i - distance, i) for i in devices if i - distance in devices]
    return lax.ppermute(block, axis, route)


def attention_kernel(kv_heads, groups, info, q_ref, a_ref, b_ref, o_ref, q_s, s_s, m_s, l_s, acc_s):
    rows = q_ref.shape[0]
    pairs = a_ref.shape[0]
    docs = info.shape[0] - 1 - 2 * pairs
    scale = HEAD_SIZE ** (-0.5)
    base = info[0]
    position = base + lax.broadcasted_iota(jnp.int32, (rows, 2 * rows), 0)
    first = jnp.zeros((rows, 2 * rows), jnp.int32)
    lowest = jnp.int32(0)
    begin = jnp.int32(0)
    for d in range(docs):
        end = begin + info[1 + 2 * pairs + d] * BLK
        first = jnp.where((position >= begin) & (position < end), begin, first)
        lowest = jnp.where((base >= begin) & (base < end), begin, lowest)
        begin = end
    limit = (position // BLK + 1) * BLK
    lane = lax.broadcasted_iota(jnp.int32, (rows, 2 * rows), 1)

    def active(p):
        low = jnp.minimum(info[1 + 2 * p], info[2 + 2 * p])
        return (low + 2 * rows > lowest) & (low < base + rows)

    for h in range(kv_heads):
        for g in range(groups):
            at = (h * groups + g) * HEAD_SIZE
            q_s[g * rows : (g + 1) * rows, :] = q_ref[:, at : at + HEAD_SIZE]
        m_s[...] = jnp.full(m_s.shape, -1e30, jnp.float32)
        l_s[...] = jnp.zeros(l_s.shape, jnp.float32)
        acc_s[...] = jnp.zeros(acc_s.shape, jnp.float32)
        k_at = h * HEAD_SIZE
        v_at = (kv_heads + h) * HEAD_SIZE

        def score(p, carry):
            @pl.when(active(p))
            def _():
                k = jnp.concatenate(
                    [a_ref[p, :, k_at : k_at + HEAD_SIZE], b_ref[p, :, k_at : k_at + HEAD_SIZE]], 0
                )
                key_pos = jnp.where(lane < rows, info[1 + 2 * p] + lane, info[2 + 2 * p] + lane - rows)
                mask = (key_pos >= first) & (key_pos < limit)
                for g in range(groups):
                    span = slice(g * rows, (g + 1) * rows)
                    s = lax.dot_general(
                        q_s[span, :], k, (((1,), (1,)), ((), ())), preferred_element_type=jnp.float32
                    )
                    s = jnp.where(mask, s * scale, -1e30)
                    s_s[p, span, :] = s
                    m_s[span, :] = jnp.maximum(m_s[span, :], jnp.maximum(s[:, :rows], s[:, rows:]))

            return carry

        lax.fori_loop(0, pairs, score, 0)
        for g in range(groups):
            span = slice(g * rows, (g + 1) * rows)
            m_s[span, :] = jnp.broadcast_to(jnp.max(m_s[span, :], axis=1, keepdims=True), (rows, rows))

        def weigh(p, carry):
            @pl.when(active(p))
            def _():
                v = jnp.concatenate(
                    [a_ref[p, :, v_at : v_at + HEAD_SIZE], b_ref[p, :, v_at : v_at + HEAD_SIZE]], 0
                )
                for g in range(groups):
                    span = slice(g * rows, (g + 1) * rows)
                    m = m_s[span, :]
                    w = jnp.exp(s_s[p, span, :] - jnp.concatenate([m, m], 1))
                    l_s[span, :] += w[:, :rows] + w[:, rows:]
                    acc_s[span, :] += jnp.dot(
                        w.astype(jnp.bfloat16), v, preferred_element_type=jnp.float32
                    )

            return carry

        lax.fori_loop(0, pairs, weigh, 0)
        for g in range(groups):
            span = slice(g * rows, (g + 1) * rows)
            at = (h * groups + g) * HEAD_SIZE
            total = jnp.sum(l_s[span, :], axis=1, keepdims=True)
            o_ref[:, at : at + HEAD_SIZE] = (acc_s[span, :] / total).astype(o_ref.dtype)


def attend(info, queries, near, far):
    rows, width = queries.shape
    kv_heads = near.shape[2] // (2 * HEAD_SIZE)
    groups = width // HEAD_SIZE // kv_heads
    pairs = near.shape[0]
    tall = groups * rows
    vmem = pl.BlockSpec(memory_space=pltpu.VMEM)
    return pl.pallas_call(
        functools.partial(attention_kernel, kv_heads, groups),
        out_shape=jax.ShapeDtypeStruct((rows, width), jnp.bfloat16),
        in_specs=[pl.BlockSpec(memory_space=pltpu.SMEM), vmem, vmem, vmem],
        out_specs=vmem,
        scratch_shapes=[
            pltpu.VMEM((tall, HEAD_SIZE), jnp.bfloat16),
            pltpu.VMEM((pairs, tall, 2 * rows), jnp.float32),
            pltpu.VMEM((tall, rows), jnp.float32),
            pltpu.VMEM((tall, rows), jnp.float32),
            pltpu.VMEM((tall, HEAD_SIZE), jnp.float32),
        ],
        cost_estimate=pl.CostEstimate(
            flops=8 * rows * width * pairs * rows,
            bytes_accessed=4 * rows * width,
            transcendentals=2 * rows * rows * pairs * width // HEAD_SIZE,
        ),
        compiler_params=pltpu.CompilerParams(vmem_limit_bytes=40 * 1024 * 1024),
        name="attend",
    )(info, queries, near, far)


def ordered(parts, bit):
    low = jnp.concatenate(parts, axis=-1)
    high = jnp.concatenate(parts[::-1], axis=-1)
    return jnp.where(bit == 0, low, high)


def on_device(
    queries, keys, values, residual, out_weight, norm_gain, level_shift, doc_lengths, noise_level
):
    rows = queries.shape[0]
    here = lax.axis_index("srv")
    devices = lax.axis_size("srv")
    sections = lax.axis_size("section")
    peers = lax.axis_size("tp")
    mine = lax.axis_index("tp")
    whole_index = lax.axis_index("section") * devices + here
    bits = devices.bit_length() - 1
    low = 1 << LOW_BITS

    kv = jnp.concatenate([keys, values], axis=1)
    turns = -(-(devices // 2) // low)
    back = [shifted(kv, "srv", low * k) for k in range(1, turns + 1)]
    beside = flipped(kv, 2)
    beside_back = flipped(jnp.stack(back), 2)
    near = jnp.concatenate([jnp.stack([kv] + back + [beside]), beside_back], axis=0)
    far = flipped(near, 1)
    own = here % low
    block = here - own
    order = [(k, 0) for k in range(turns + 1)] + [(k, 2) for k in range(turns + 1)]
    spots = []
    for k, x in order:
        for c in (0, 1):
            spots.append((block - low * k + (own ^ (x + c))) * rows)
    info = jnp.stack([here * rows] + spots).astype(jnp.int32)
    info = jnp.concatenate([info, doc_lengths[0].astype(jnp.int32)])

    held = {0: out_weight}
    for b in range(3, bits):
        held.update({r | (1 << b): flipped(w, 1 << b) for r, w in list(held.items())})
    hop = 1
    while hop < sections:
        held.update(
            {r | (hop * devices): flipped(w, hop, "section") for r, w in list(held.items())}
        )
        hop *= 2
    held.update({r | 1: flipped(w, 1) for r, w in list(held.items())})

    attended = attend(info, queries, near, far)
    gathered = {0: attended}
    for r in (2, 4, 6):
        gathered[r] = flipped(attended, r)
    row_keys = (0, 2, 4, 6)
    stacked = jnp.concatenate([gathered[r] for r in row_keys], axis=0)

    span = sections * devices // peers
    by_part = []
    for part in range(peers):
        lower = sorted(r for r in held if r // span == part)
        by_part.append([jnp.dot(stacked, held[r], preferred_element_type=jnp.float32) for r in lower])
    lower = sorted(r % span for r in held if r // span == 0)
    turn = whole_index // span ^ mine

    def chosen(e):
        out = []
        for i in range(len(lower)):
            value = by_part[0][i]
            for part in range(1, peers):
                value = jnp.where((turn ^ e) == part, by_part[part][i], value)
            out.append(value)
        return jnp.concatenate(out, axis=1)

    total = chosen(0)
    for e in range(1, peers):
        total = total + flipped(chosen(e).astype(jnp.bfloat16), e, "tp").astype(jnp.float32)

    width = out_weight.shape[1]
    pieces = {}
    for i, r in enumerate(row_keys):
        piece = total[i * rows : (i + 1) * rows]
        if r:
            piece = flipped(piece.astype(jnp.bfloat16), r).astype(jnp.float32)
        for j, a in enumerate(lower):
            pieces[a ^ r] = piece[:, j * width : (j + 1) * width]
    b = 1
    while len(pieces) > 1:
        pieces = {
            r: ordered([pieces[r], pieces[r | b]], (whole_index // b) % 2)
            for r in pieces
            if not r & b
        }
        b *= 2
    hidden = pieces[0] + residual.astype(jnp.float32)

    squares = jnp.sum(hidden * hidden, axis=1, keepdims=True)
    squares = lax.psum(squares, "tp")
    inverse = lax.rsqrt(squares / (hidden.shape[1] * peers) + 1e-06)
    lengths = doc_lengths[0] * BLK
    ends = jnp.cumsum(lengths)
    starts = ends - lengths
    positions = here * rows + jnp.arange(rows, dtype=jnp.int32)
    member = (positions[:, None] >= starts[None, :]) & (positions[:, None] < ends[None, :])
    level = jnp.sum(jnp.where(member, noise_level[0][None, :], 0), axis=1)
    onehot = (level[:, None] == jnp.arange(level_shift.shape[0], dtype=jnp.int32)[None, :]).astype(
        jnp.float32
    )
    shift = jnp.dot(onehot, level_shift, precision=lax.Precision.HIGHEST)
    normed = hidden * inverse * norm_gain[None, :] * (1.0 + shift)
    return normed.astype(jnp.bfloat16)


def solution(mesh):
    placed = (
        P(("section", "srv"), "tp"),
        P(("section", "srv"), "tp"),
        P(("section", "srv"), "tp"),
        P(("section", "srv"), "tp"),
        P("tp", ("section", "srv")),
        P("tp"),
        P(None, "tp"),
        P("section", None),
        P("section", None),
    )
    return jax.shard_map(
        on_device,
        mesh=mesh,
        in_specs=placed,
        out_specs=P(("section", "srv"), "tp"),
        check_vma=False,
    )
```

```python
import functools
import jax
import jax.numpy as jnp
from jax import lax
from jax.experimental import pallas as pl
from jax.experimental.pallas import tpu as pltpu
from jax.sharding import PartitionSpec as P


HEAD_SIZE = 128
BLK = 16
LOW_BITS = 2
FIRST_STRETCHES = 2


def flipped(block, mask, axis="srv"):
    devices = range(lax.axis_size(axis))
    return lax.ppermute(block, axis, [(i, i ^ mask) for i in devices])


def shifted(block, axis, distance):
    devices = range(lax.axis_size(axis))
    route = [(i - distance, i) for i in devices if i - distance in devices]
    return lax.ppermute(block, axis, route)


def attention_kernel(kv_heads, groups, info, q_ref, a_ref, b_ref, o_ref, q_s, s_s, m_s, l_s, acc_s):
    rows = q_ref.shape[0]
    pairs = a_ref.shape[0]
    docs = info.shape[0] - 1 - 2 * pairs
    scale = HEAD_SIZE ** (-0.5)
    base = info[0]
    position = base + lax.broadcasted_iota(jnp.int32, (rows, 2 * rows), 0)
    first = jnp.zeros((rows, 2 * rows), jnp.int32)
    lowest = jnp.int32(0)
    begin = jnp.int32(0)
    for d in range(docs):
        end = begin + info[1 + 2 * pairs + d] * BLK
        first = jnp.where((position >= begin) & (position < end), begin, first)
        lowest = jnp.where((base >= begin) & (base < end), begin, lowest)
        begin = end
    limit = (position // BLK + 1) * BLK
    lane = lax.broadcasted_iota(jnp.int32, (rows, 2 * rows), 1)

    def active(p):
        low = jnp.minimum(info[1 + 2 * p], info[2 + 2 * p])
        return (low + 2 * rows > lowest) & (low < base + rows)

    for h in range(kv_heads):
        for g in range(groups):
            at = (h * groups + g) * HEAD_SIZE
            q_s[g * rows : (g + 1) * rows, :] = q_ref[:, at : at + HEAD_SIZE]
        m_s[...] = jnp.full(m_s.shape, -1e30, jnp.float32)
        l_s[...] = jnp.zeros(l_s.shape, jnp.float32)
        acc_s[...] = jnp.zeros(acc_s.shape, jnp.float32)
        k_at = h * HEAD_SIZE
        v_at = (kv_heads + h) * HEAD_SIZE

        def score(p, carry):
            @pl.when(active(p))
            def _():
                k = jnp.concatenate(
                    [a_ref[p, :, k_at : k_at + HEAD_SIZE], b_ref[p, :, k_at : k_at + HEAD_SIZE]], 0
                )
                key_pos = jnp.where(lane < rows, info[1 + 2 * p] + lane, info[2 + 2 * p] + lane - rows)
                mask = (key_pos >= first) & (key_pos < limit)
                for g in range(groups):
                    span = slice(g * rows, (g + 1) * rows)
                    s = lax.dot_general(
                        q_s[span, :], k, (((1,), (1,)), ((), ())), preferred_element_type=jnp.float32
                    )
                    s = jnp.where(mask, s * scale, -1e30)
                    s_s[p, span, :] = s
                    m_s[span, :] = jnp.maximum(m_s[span, :], jnp.maximum(s[:, :rows], s[:, rows:]))

            return carry

        lax.fori_loop(0, pairs, score, 0)
        for g in range(groups):
            span = slice(g * rows, (g + 1) * rows)
            m_s[span, :] = jnp.broadcast_to(jnp.max(m_s[span, :], axis=1, keepdims=True), (rows, rows))

        def weigh(p, carry):
            @pl.when(active(p))
            def _():
                v = jnp.concatenate(
                    [a_ref[p, :, v_at : v_at + HEAD_SIZE], b_ref[p, :, v_at : v_at + HEAD_SIZE]], 0
                )
                for g in range(groups):
                    span = slice(g * rows, (g + 1) * rows)
                    m = m_s[span, :]
                    w = jnp.exp(s_s[p, span, :] - jnp.concatenate([m, m], 1))
                    l_s[span, :] += w[:, :rows] + w[:, rows:]
                    acc_s[span, :] += jnp.dot(
                        w.astype(jnp.bfloat16), v, preferred_element_type=jnp.float32
                    )

            return carry

        lax.fori_loop(0, pairs, weigh, 0)
        for g in range(groups):
            span = slice(g * rows, (g + 1) * rows)
            at = (h * groups + g) * HEAD_SIZE
            total = jnp.sum(l_s[span, :], axis=1, keepdims=True)
            o_ref[:, at : at + HEAD_SIZE] = (acc_s[span, :] / total).astype(o_ref.dtype)


def attend(info, queries, near, far):
    rows, width = queries.shape
    kv_heads = near.shape[2] // (2 * HEAD_SIZE)
    groups = width // HEAD_SIZE // kv_heads
    pairs = near.shape[0]
    tall = groups * rows
    vmem = pl.BlockSpec(memory_space=pltpu.VMEM)
    return pl.pallas_call(
        functools.partial(attention_kernel, kv_heads, groups),
        out_shape=jax.ShapeDtypeStruct((rows, width), jnp.bfloat16),
        in_specs=[pl.BlockSpec(memory_space=pltpu.SMEM), vmem, vmem, vmem],
        out_specs=vmem,
        scratch_shapes=[
            pltpu.VMEM((tall, HEAD_SIZE), jnp.bfloat16),
            pltpu.VMEM((pairs, tall, 2 * rows), jnp.float32),
            pltpu.VMEM((tall, rows), jnp.float32),
            pltpu.VMEM((tall, rows), jnp.float32),
            pltpu.VMEM((tall, HEAD_SIZE), jnp.float32),
        ],
        cost_estimate=pl.CostEstimate(
            flops=8 * rows * width * pairs * rows,
            bytes_accessed=4 * rows * width,
            transcendentals=2 * rows * rows * pairs * width // HEAD_SIZE,
        ),
        compiler_params=pltpu.CompilerParams(vmem_limit_bytes=40 * 1024 * 1024),
        name="attend",
    )(info, queries, near, far)


def ordered(parts, bit):
    low = jnp.concatenate(parts, axis=-1)
    high = jnp.concatenate(parts[::-1], axis=-1)
    return jnp.where(bit == 0, low, high)


def project_kernel(count, layout, cut, *refs):
    rows = refs[:count]
    arrays = refs[count:-1]
    out = refs[-1]
    columns = []
    for segments in layout:
        taken = [arrays[n][:, at : at + cut] for n, at in segments]
        columns.append(taken[0] if len(taken) == 1 else jnp.concatenate(taken, axis=0))
    w = columns[0] if len(columns) == 1 else jnp.concatenate(columns, axis=1)
    size = rows[0].shape[0]
    for i in range(count):
        out[i * size : (i + 1) * size, :] = jnp.dot(
            rows[i][...], w, preferred_element_type=jnp.float32
        ).astype(out.dtype)


def project(rows, parts, cut):
    height = sum(r.shape[0] for r in rows)
    depth = rows[0].shape[1]
    width = cut * len(parts)
    if cut % 128:
        columns = [
            jnp.concatenate([w[:, at : at + cut] for w, at in segments], 0) for segments in parts
        ]
        joined = jnp.dot(
            jnp.concatenate(rows, 0), jnp.concatenate(columns, 1), preferred_element_type=jnp.float32
        )
        return joined.astype(jnp.bfloat16)
    arrays = [w for segments in parts for w, _ in segments]
    layout, n = [], 0
    for segments in parts:
        layout.append(tuple((n + i, at) for i, (_, at) in enumerate(segments)))
        n += len(segments)
    vmem = pl.BlockSpec(memory_space=pltpu.VMEM)
    return pl.pallas_call(
        functools.partial(project_kernel, len(rows), tuple(layout), cut),
        out_shape=jax.ShapeDtypeStruct((height, width), jnp.bfloat16),
        in_specs=[vmem] * (len(rows) + len(arrays)),
        out_specs=vmem,
        cost_estimate=pl.CostEstimate(
            flops=2 * height * width * depth,
            bytes_accessed=2 * depth * (height + width),
            transcendentals=0,
        ),
        compiler_params=pltpu.CompilerParams(vmem_limit_bytes=24 * 1024 * 1024),
        name="project",
    )(*rows, *arrays)


def on_device(
    queries, keys, values, residual, out_weight, norm_gain, level_shift, doc_lengths, noise_level
):
    rows = queries.shape[0]
    here = lax.axis_index("srv")
    devices = lax.axis_size("srv")
    sections = lax.axis_size("section")
    peers = lax.axis_size("tp")
    mine = lax.axis_index("tp")
    whole_index = lax.axis_index("section") * devices + here
    bits = devices.bit_length() - 1
    low = 1 << LOW_BITS
    width = out_weight.shape[1]
    chunks = max(1, width // 128)
    cut = width // chunks

    kv = jnp.concatenate([keys, values], axis=1)
    turns = -(-(devices // 2) // low)
    back = []
    for k in range(1, turns + 1):
        back.append(shifted(kv, "srv", low * k))
    beside = flipped(kv, 2)
    beside_back = flipped(jnp.stack(back), 2)
    near = jnp.concatenate([jnp.stack([kv] + back + [beside]), beside_back], axis=0)
    far = flipped(near, 1)
    own = here % low
    block = here - own
    order = [(k, 0) for k in range(turns + 1)] + [(k, 2) for k in range(turns + 1)]
    spots = []
    for k, x in order:
        for c in (0, 1):
            spots.append((block - low * k + (own ^ (x + c))) * rows)
    info = jnp.stack([here * rows] + spots).astype(jnp.int32)
    info = jnp.concatenate([info, doc_lengths[0].astype(jnp.int32)])

    depth = out_weight.shape[0]
    pieces_of = []
    for j in range(chunks):
        stretches = FIRST_STRETCHES if j == 0 else 1
        pieces_of.append([(j, n, depth // stretches) for n in range(stretches)])
    held = []
    for j in range(chunks):
        segments = []
        for _, n, size in pieces_of[j]:
            got = {0: out_weight[n * size : (n + 1) * size, j * cut : (j + 1) * cut]}
            for b in range(3, bits):
                got.update({r | (1 << b): flipped(w, 1 << b) for r, w in list(got.items())})
            hop = 1
            while hop < sections:
                got.update(
                    {r | (hop * devices): flipped(w, hop, "section") for r, w in list(got.items())}
                )
                hop *= 2
            segments.append(got)
        held.append(segments)
    beside_own = flipped(out_weight, 1)
    sources = []
    for j in range(chunks):
        found = {0: [(out_weight, j * cut)], 1: [(beside_own, j * cut)]}
        for got in held[j]:
            for r, w in got.items():
                if r:
                    found.setdefault(r, []).append((w, 0))
                    found.setdefault(r | 1, []).append((flipped(w, 1), 0))
        sources.append(found)

    attended = attend(info, queries, near, far)
    row_keys = (0, 2, 4, 6)
    across = flipped(attended, 4)
    gathered = [attended, flipped(attended, 2), across]
    gathered.append(flipped(across, 2))

    lengths = doc_lengths[0] * BLK
    ends = jnp.cumsum(lengths)
    starts = ends - lengths
    positions = here * rows + jnp.arange(rows, dtype=jnp.int32)
    member = (positions[:, None] >= starts[None, :]) & (positions[:, None] < ends[None, :])
    level = jnp.sum(jnp.where(member, noise_level[0][None, :], 0), axis=1)
    onehot = (level[:, None] == jnp.arange(level_shift.shape[0], dtype=jnp.int32)[None, :]).astype(
        jnp.float32
    )
    shift = jnp.dot(onehot, level_shift, precision=lax.Precision.HIGHEST)
    factor = norm_gain[None, :] * (1.0 + shift)
    base, factor, gathered[1] = lax.optimization_barrier(
        (residual.astype(jnp.float32), factor, gathered[1])
    )

    span = sections * devices // peers
    turn = whole_index // span ^ mine
    lower = sorted(r for r in sources[0] if r < span)
    pieces = {}
    for j in range(chunks):
        by_part = [
            project(gathered, [sources[j][part * span + r] for r in lower], cut)
            for part in range(peers)
        ]

        def chosen(e):
            value = by_part[0]
            for part in range(1, peers):
                value = jnp.where((turn ^ e) == part, by_part[part], value)
            return value

        total = chosen(0).astype(jnp.float32)
        for e in range(1, peers):
            total = total + flipped(chosen(e), e, "tp").astype(jnp.float32)
        for i, r in enumerate(row_keys):
            piece = total[i * rows : (i + 1) * rows]
            if r:
                piece = flipped(piece.astype(jnp.bfloat16), r).astype(jnp.float32)
            for n, a in enumerate(lower):
                pieces.setdefault(a ^ r, []).append(piece[:, n * cut : (n + 1) * cut])
    pieces = {r: jnp.concatenate(p, axis=1) for r, p in pieces.items()}
    b = 1
    while len(pieces) > 1:
        pieces = {
            r: ordered([pieces[r], pieces[r | b]], (whole_index // b) % 2)
            for r in pieces
            if not r & b
        }
        b *= 2
    hidden = pieces[0] + base

    squares = jnp.sum(hidden * hidden, axis=1)
    hop = 1
    while hop < peers:
        squares = squares + flipped(squares, hop, "tp")
        hop *= 2
    inverse = lax.rsqrt(squares / (hidden.shape[1] * peers) + 1e-06)[:, None]
    normed = hidden * inverse * factor
    return normed.astype(jnp.bfloat16)


def solution(mesh):
    placed = (
        P(("section", "srv"), "tp"),
        P(("section", "srv"), "tp"),
        P(("section", "srv"), "tp"),
        P(("section", "srv"), "tp"),
        P("tp", ("section", "srv")),
        P("tp"),
        P(None, "tp"),
        P("section", None),
        P("section", None),
    )
    return jax.shard_map(
        on_device,
        mesh=mesh,
        in_specs=placed,
        out_specs=P(("section", "srv"), "tp"),
        check_vma=False,
    )
```

```python
import functools
import jax
import jax.numpy as jnp
from jax import lax
from jax.experimental import pallas as pl
from jax.experimental.pallas import tpu as pltpu
from jax.sharding import PartitionSpec as P


HEAD_SIZE = 128
BLK = 16
LOW_BITS = 2
FIRST_STRETCHES = (3, 1)


def flipped(block, mask, axis="srv"):
    devices = range(lax.axis_size(axis))
    return lax.ppermute(block, axis, [(i, i ^ mask) for i in devices])


def shifted(block, axis, distance):
    devices = range(lax.axis_size(axis))
    route = [(i - distance, i) for i in devices if i - distance in devices]
    return lax.ppermute(block, axis, route)


def attention_kernel(kv_heads, h, info, q_ref, a_ref, b_ref, o_ref, s_s, m_s, l_s, acc_s):
    groups, rows, _ = q_ref.shape
    pairs = a_ref.shape[0]
    docs = info.shape[0] - 1 - 2 * pairs
    scale = HEAD_SIZE ** (-0.5)
    base = info[0]
    position = base + lax.broadcasted_iota(jnp.int32, (rows, 2 * rows), 0)
    first = jnp.zeros((rows, 2 * rows), jnp.int32)
    lowest = jnp.int32(0)
    begin = jnp.int32(0)
    for d in range(docs):
        end = begin + info[1 + 2 * pairs + d] * BLK
        first = jnp.where((position >= begin) & (position < end), begin, first)
        lowest = jnp.where((base >= begin) & (base < end), begin, lowest)
        begin = end
    limit = (position // BLK + 1) * BLK
    lane = lax.broadcasted_iota(jnp.int32, (rows, 2 * rows), 1)
    k_at = h * HEAD_SIZE
    v_at = (kv_heads + h) * HEAD_SIZE
    m_s[...] = jnp.full(m_s.shape, -1e30, jnp.float32)
    l_s[...] = jnp.zeros(l_s.shape, jnp.float32)
    acc_s[...] = jnp.zeros(acc_s.shape, jnp.float32)

    def active(p):
        low = jnp.minimum(info[1 + 2 * p], info[2 + 2 * p])
        return (low + 2 * rows > lowest) & (low < base + rows)

    def score(p, carry):
        @pl.when(active(p))
        def _():
            k = jnp.concatenate(
                [a_ref[p, :, k_at : k_at + HEAD_SIZE], b_ref[p, :, k_at : k_at + HEAD_SIZE]], 0
            )
            key_pos = jnp.where(lane < rows, info[1 + 2 * p] + lane, info[2 + 2 * p] + lane - rows)
            mask = (key_pos >= first) & (key_pos < limit)
            for g in range(groups):
                s = lax.dot_general(
                    q_ref[g], k, (((1,), (1,)), ((), ())), preferred_element_type=jnp.float32
                )
                s = jnp.where(mask, s * scale, -1e30)
                s_s[p, g] = s
                m_s[g] = jnp.maximum(m_s[g], jnp.maximum(s[:, :rows], s[:, rows:]))

        return carry

    lax.fori_loop(0, pairs, score, 0)
    for g in range(groups):
        m_s[g] = jnp.broadcast_to(jnp.max(m_s[g], axis=1, keepdims=True), (rows, rows))

    def weigh(p, carry):
        @pl.when(active(p))
        def _():
            v = jnp.concatenate(
                [a_ref[p, :, v_at : v_at + HEAD_SIZE], b_ref[p, :, v_at : v_at + HEAD_SIZE]], 0
            )
            for g in range(groups):
                m = m_s[g]
                w = jnp.exp(s_s[p, g] - jnp.concatenate([m, m], 1))
                l_s[g] += w[:, :rows] + w[:, rows:]
                acc_s[g] += jnp.dot(w.astype(jnp.bfloat16), v, preferred_element_type=jnp.float32)

        return carry

    lax.fori_loop(0, pairs, weigh, 0)
    for g in range(groups):
        at = g * HEAD_SIZE
        total = jnp.sum(l_s[g], axis=1, keepdims=True)
        o_ref[:, at : at + HEAD_SIZE] = (acc_s[g] / total).astype(o_ref.dtype)


def attend(info, queries, near, far, kv_heads, h):
    groups, rows, _ = queries.shape
    pairs = near.shape[0]
    vmem = pl.BlockSpec(memory_space=pltpu.VMEM)
    return pl.pallas_call(
        functools.partial(attention_kernel, kv_heads, h),
        out_shape=jax.ShapeDtypeStruct((rows, groups * HEAD_SIZE), jnp.bfloat16),
        in_specs=[pl.BlockSpec(memory_space=pltpu.SMEM), vmem, vmem, vmem],
        out_specs=vmem,
        scratch_shapes=[
            pltpu.VMEM((pairs, groups, rows, 2 * rows), jnp.float32),
            pltpu.VMEM((groups, rows, rows), jnp.float32),
            pltpu.VMEM((groups, rows, rows), jnp.float32),
            pltpu.VMEM((groups, rows, HEAD_SIZE), jnp.float32),
        ],
        cost_estimate=pl.CostEstimate(
            flops=8 * rows * groups * HEAD_SIZE * pairs * rows,
            bytes_accessed=4 * rows * groups * HEAD_SIZE,
            transcendentals=2 * rows * rows * pairs * groups,
        ),
        compiler_params=pltpu.CompilerParams(vmem_limit_bytes=32 * 1024 * 1024),
        name="attend",
    )(info, queries, near, far)


def ordered(parts, bit):
    low = jnp.concatenate(parts, axis=-1)
    high = jnp.concatenate(parts[::-1], axis=-1)
    return jnp.where(bit == 0, low, high)


def project_kernel(count, halves, layout, cut, *refs):
    rows = [refs[i * halves : (i + 1) * halves] for i in range(count)]
    arrays = refs[count * halves : -1]
    out = refs[-1]
    columns = []
    for segments in layout:
        taken = [arrays[n][:, at : at + cut] for n, at in segments]
        columns.append(taken[0] if len(taken) == 1 else jnp.concatenate(taken, axis=0))
    w = columns[0] if len(columns) == 1 else jnp.concatenate(columns, axis=1)
    size = rows[0][0].shape[0]
    for i in range(count):
        x = jnp.concatenate([r[...] for r in rows[i]], axis=1)
        out[i * size : (i + 1) * size, :] = jnp.dot(
            x, w, preferred_element_type=jnp.float32
        ).astype(out.dtype)


def project(rows, parts, cut):
    halves = len(rows[0])
    height = sum(r[0].shape[0] for r in rows)
    depth = sum(x.shape[1] for x in rows[0])
    width = cut * len(parts)
    flat = [x for r in rows for x in r]
    if cut % 128:
        columns = [
            jnp.concatenate([w[:, at : at + cut] for w, at in segments], 0) for segments in parts
        ]
        joined = jnp.dot(
            jnp.concatenate([jnp.concatenate(r, 1) for r in rows], 0),
            jnp.concatenate(columns, 1),
            preferred_element_type=jnp.float32,
        )
        return joined.astype(jnp.bfloat16)
    arrays = [w for segments in parts for w, _ in segments]
    layout, n = [], 0
    for segments in parts:
        layout.append(tuple((n + i, at) for i, (_, at) in enumerate(segments)))
        n += len(segments)
    vmem = pl.BlockSpec(memory_space=pltpu.VMEM)
    return pl.pallas_call(
        functools.partial(project_kernel, len(rows), halves, tuple(layout), cut),
        out_shape=jax.ShapeDtypeStruct((height, width), jnp.bfloat16),
        in_specs=[vmem] * (len(flat) + len(arrays)),
        out_specs=vmem,
        cost_estimate=pl.CostEstimate(
            flops=2 * height * width * depth,
            bytes_accessed=2 * depth * (height + width),
            transcendentals=0,
        ),
        compiler_params=pltpu.CompilerParams(vmem_limit_bytes=24 * 1024 * 1024),
        name="project",
    )(*flat, *arrays)


def on_device(
    queries, keys, values, residual, out_weight, norm_gain, level_shift, doc_lengths, noise_level
):
    rows = queries.shape[0]
    here = lax.axis_index("srv")
    devices = lax.axis_size("srv")
    sections = lax.axis_size("section")
    peers = lax.axis_size("tp")
    mine = lax.axis_index("tp")
    whole_index = lax.axis_index("section") * devices + here
    bits = devices.bit_length() - 1
    low = 1 << LOW_BITS
    width = out_weight.shape[1]
    chunks = max(1, width // 128)
    cut = width // chunks

    kv = jnp.concatenate([keys, values], axis=1)
    turns = -(-(devices // 2) // low)
    back = []
    for k in range(1, turns + 1):
        back.append(shifted(kv, "srv", low * k))
    beside = flipped(kv, 2)
    beside_back = flipped(jnp.stack(back), 2)
    own = here % low
    block = here - own
    order = [(k, 0) for k in range(turns + 1)] + [(k, 2) for k in range(turns + 1)]
    spots = []
    for k, x in order:
        for c in (0, 1):
            spots.append((block - low * k + (own ^ (x + c))) * rows)
    info = jnp.stack([here * rows] + spots).astype(jnp.int32)
    info = jnp.concatenate([info, doc_lengths[0].astype(jnp.int32)])
    by_head = queries.reshape(rows, -1, HEAD_SIZE).transpose(1, 0, 2)
    beside_back, by_head, info = lax.optimization_barrier((beside_back, by_head, info))
    near = jnp.concatenate([jnp.stack([kv] + back + [beside]), beside_back], axis=0)
    far = flipped(near, 1)

    depth = out_weight.shape[0]
    pieces_of = []
    for j in range(chunks):
        shares = FIRST_STRETCHES if j == 0 else (1,)
        unit = depth // sum(shares)
        pieces_of.append([(n, sum(shares[:n]) * unit, share * unit) for n, share in enumerate(shares)])
    held = []
    for j in range(chunks):
        segments = []
        for n, at, size in pieces_of[j]:
            got = {0: out_weight[at : at + size, j * cut : (j + 1) * cut]}
            for b in range(3, bits):
                got.update({r | (1 << b): flipped(w, 1 << b) for r, w in list(got.items())})
            hop = 1
            while hop < sections:
                got.update(
                    {r | (hop * devices): flipped(w, hop, "section") for r, w in list(got.items())}
                )
                hop *= 2
            segments.append(got)
        held.append(segments)
    beside_own = flipped(out_weight, 1)
    sources = []
    for j in range(chunks):
        found = {0: [(out_weight, j * cut)], 1: [(beside_own, j * cut)]}
        for got in held[j]:
            for r, w in got.items():
                if r:
                    found.setdefault(r, []).append((w, 0))
                    found.setdefault(r | 1, []).append((flipped(w, 1), 0))
        sources.append(found)

    kv_heads = keys.shape[1] // HEAD_SIZE
    groups = by_head.shape[0] // kv_heads
    attended, across = [], []
    for h in range(kv_heads):
        attended.append(
            attend(info, by_head[h * groups : (h + 1) * groups], near, far, kv_heads, h)
        )
        across.append(flipped(attended[h], 4))
    row_keys = (0, 2, 4, 6)
    beside_rows, cross_rows = [], []
    for h in range(kv_heads):
        beside_rows.append(flipped(attended[h], 2))
        cross_rows.append(flipped(across[h], 2))
    gathered = [attended, beside_rows, across, cross_rows]

    lengths = doc_lengths[0] * BLK
    ends = jnp.cumsum(lengths)
    starts = ends - lengths
    positions = here * rows + jnp.arange(rows, dtype=jnp.int32)
    member = (positions[:, None] >= starts[None, :]) & (positions[:, None] < ends[None, :])
    level = jnp.sum(jnp.where(member, noise_level[0][None, :], 0), axis=1)
    onehot = (level[:, None] == jnp.arange(level_shift.shape[0], dtype=jnp.int32)[None, :]).astype(
        jnp.float32
    )
    shift = jnp.dot(onehot, level_shift, precision=lax.Precision.HIGHEST)
    factor = norm_gain[None, :] * (1.0 + shift)
    blocks = residual.shape[1] // width
    residuals = [
        jnp.concatenate(
            [residual[:, b * width + j * cut : b * width + (j + 1) * cut] for b in range(blocks)], 1
        )
        for j in range(chunks)
    ]
    factor, residuals, beside_rows[0] = lax.optimization_barrier(
        (factor, residuals, beside_rows[0])
    )

    span = sections * devices // peers
    turn = whole_index // span ^ mine
    lower = sorted(r for r in sources[0] if r < span)
    hidden, squares = [], 0.0
    for j in range(chunks):
        by_part = []
        pieces = {}
        for part in range(peers):
            by_part.append(
                project(gathered, [sources[j][part * span + r] for r in lower], cut)
            )

        def chosen(e):
            value = by_part[0]
            for part in range(1, peers):
                value = jnp.where((turn ^ e) == part, by_part[part], value)
            return value

        total = chosen(0).astype(jnp.float32)
        for e in range(1, peers):
            total = total + flipped(chosen(e), e, "tp").astype(jnp.float32)
        for i, r in enumerate(row_keys):
            piece = total[i * rows : (i + 1) * rows]
            if r:
                piece = flipped(piece.astype(jnp.bfloat16), r).astype(jnp.float32)
            for n, a in enumerate(lower):
                pieces[a ^ r] = piece[:, n * cut : (n + 1) * cut]
        b = 1
        while len(pieces) > 1:
            pieces = {
                r: ordered([pieces[r], pieces[r | b]], (whole_index // b) % 2)
                for r in pieces
                if not r & b
            }
            b *= 2
        hidden.append(pieces[0] + residuals[j].astype(jnp.float32))
        squares = squares + jnp.sum(hidden[j] * hidden[j], axis=1)

    hop = 1
    while hop < peers:
        squares = squares + flipped(squares, hop, "tp")
        hop *= 2
    inverse = lax.rsqrt(squares / (residual.shape[1] * peers) + 1e-06)[:, None]
    normed = jnp.concatenate(
        [hidden[j][:, b * cut : (b + 1) * cut] for b in range(blocks) for j in range(chunks)], axis=1
    )
    return (normed * inverse * factor).astype(jnp.bfloat16)


def solution(mesh):
    placed = (
        P(("section", "srv"), "tp"),
        P(("section", "srv"), "tp"),
        P(("section", "srv"), "tp"),
        P(("section", "srv"), "tp"),
        P("tp", ("section", "srv")),
        P("tp"),
        P(None, "tp"),
        P("section", None),
        P("section", None),
    )
    return jax.shard_map(
        on_device,
        mesh=mesh,
        in_specs=placed,
        out_specs=P(("section", "srv"), "tp"),
        check_vma=False,
    )
```

```python
import functools
import jax
import jax.numpy as jnp
from jax import lax
from jax.experimental import pallas as pl
from jax.experimental.pallas import tpu as pltpu
from jax.sharding import PartitionSpec as P


HEAD_SIZE = 128
BLK = 16
LOW_BITS = 2
FIRST_STRETCHES = (15, 1)


def flipped(block, mask, axis="srv"):
    devices = range(lax.axis_size(axis))
    return lax.ppermute(block, axis, [(i, i ^ mask) for i in devices])


def shifted(block, axis, distance):
    devices = range(lax.axis_size(axis))
    route = [(i - distance, i) for i in devices if i - distance in devices]
    return lax.ppermute(block, axis, route)


def attention_kernel(kv_heads, h, info, q_ref, a_ref, b_ref, o_ref, s_s, m_s, l_s, acc_s):
    groups, rows, _ = q_ref.shape
    pairs = a_ref.shape[0]
    docs = info.shape[0] - 1 - 2 * pairs
    scale = HEAD_SIZE ** (-0.5)
    base = info[0]
    position = base + lax.broadcasted_iota(jnp.int32, (rows, 2 * rows), 0)
    first = jnp.zeros((rows, 2 * rows), jnp.int32)
    lowest = jnp.int32(0)
    begin = jnp.int32(0)
    for d in range(docs):
        end = begin + info[1 + 2 * pairs + d] * BLK
        first = jnp.where((position >= begin) & (position < end), begin, first)
        lowest = jnp.where((base >= begin) & (base < end), begin, lowest)
        begin = end
    limit = (position // BLK + 1) * BLK
    lane = lax.broadcasted_iota(jnp.int32, (rows, 2 * rows), 1)
    k_at = h * HEAD_SIZE
    v_at = (kv_heads + h) * HEAD_SIZE
    m_s[...] = jnp.full(m_s.shape, -1e30, jnp.float32)
    l_s[...] = jnp.zeros(l_s.shape, jnp.float32)
    acc_s[...] = jnp.zeros(acc_s.shape, jnp.float32)

    def active(p):
        low = jnp.minimum(info[1 + 2 * p], info[2 + 2 * p])
        return (low + 2 * rows > lowest) & (low < base + rows)

    def score(p, carry):
        @pl.when(active(p))
        def _():
            k = jnp.concatenate(
                [a_ref[p, :, k_at : k_at + HEAD_SIZE], b_ref[p, :, k_at : k_at + HEAD_SIZE]], 0
            )
            key_pos = jnp.where(lane < rows, info[1 + 2 * p] + lane, info[2 + 2 * p] + lane - rows)
            mask = (key_pos >= first) & (key_pos < limit)
            for g in range(groups):
                s = lax.dot_general(
                    q_ref[g], k, (((1,), (1,)), ((), ())), preferred_element_type=jnp.float32
                )
                s = jnp.where(mask, s * scale, -1e30)
                s_s[p, g] = s
                m_s[g] = jnp.maximum(m_s[g], jnp.maximum(s[:, :rows], s[:, rows:]))

        return carry

    lax.fori_loop(0, pairs, score, 0)
    for g in range(groups):
        m_s[g] = jnp.broadcast_to(jnp.max(m_s[g], axis=1, keepdims=True), (rows, rows))

    def weigh(p, carry):
        @pl.when(active(p))
        def _():
            v = jnp.concatenate(
                [a_ref[p, :, v_at : v_at + HEAD_SIZE], b_ref[p, :, v_at : v_at + HEAD_SIZE]], 0
            )
            for g in range(groups):
                m = m_s[g]
                w = jnp.exp(s_s[p, g] - jnp.concatenate([m, m], 1))
                l_s[g] += w[:, :rows] + w[:, rows:]
                acc_s[g] += jnp.dot(w.astype(jnp.bfloat16), v, preferred_element_type=jnp.float32)

        return carry

    lax.fori_loop(0, pairs, weigh, 0)
    for g in range(groups):
        at = g * HEAD_SIZE
        total = jnp.sum(l_s[g], axis=1, keepdims=True)
        o_ref[:, at : at + HEAD_SIZE] = (acc_s[g] / total).astype(o_ref.dtype)


def attend(info, queries, near, far, kv_heads, h):
    groups, rows, _ = queries.shape
    pairs = near.shape[0]
    vmem = pl.BlockSpec(memory_space=pltpu.VMEM)
    return pl.pallas_call(
        functools.partial(attention_kernel, kv_heads, h),
        out_shape=jax.ShapeDtypeStruct((rows, groups * HEAD_SIZE), jnp.bfloat16),
        in_specs=[pl.BlockSpec(memory_space=pltpu.SMEM), vmem, vmem, vmem],
        out_specs=vmem,
        scratch_shapes=[
            pltpu.VMEM((pairs, groups, rows, 2 * rows), jnp.float32),
            pltpu.VMEM((groups, rows, rows), jnp.float32),
            pltpu.VMEM((groups, rows, rows), jnp.float32),
            pltpu.VMEM((groups, rows, HEAD_SIZE), jnp.float32),
        ],
        cost_estimate=pl.CostEstimate(
            flops=8 * rows * groups * HEAD_SIZE * pairs * rows,
            bytes_accessed=4 * rows * groups * HEAD_SIZE,
            transcendentals=2 * rows * rows * pairs * groups,
        ),
        compiler_params=pltpu.CompilerParams(vmem_limit_bytes=32 * 1024 * 1024),
        name="attend",
    )(info, queries, near, far)


def ordered(parts, bit):
    low = jnp.concatenate(parts, axis=-1)
    high = jnp.concatenate(parts[::-1], axis=-1)
    return jnp.where(bit == 0, low, high)


def project_kernel(count, halves, layout, cut, *refs):
    rows = [refs[i * halves : (i + 1) * halves] for i in range(count)]
    arrays = refs[count * halves : -1]
    out = refs[-1]
    columns = []
    for segments in layout:
        taken = [arrays[n][:, at : at + cut] for n, at in segments]
        columns.append(taken[0] if len(taken) == 1 else jnp.concatenate(taken, axis=0))
    w = columns[0] if len(columns) == 1 else jnp.concatenate(columns, axis=1)
    size = rows[0][0].shape[0]
    for i in range(count):
        x = jnp.concatenate([r[...] for r in rows[i]], axis=1)
        out[i * size : (i + 1) * size, :] = jnp.dot(
            x, w, preferred_element_type=jnp.float32
        ).astype(out.dtype)


def project(rows, parts, cut):
    halves = len(rows[0])
    height = sum(r[0].shape[0] for r in rows)
    depth = sum(x.shape[1] for x in rows[0])
    width = cut * len(parts)
    flat = [x for r in rows for x in r]
    if cut % 128:
        columns = [
            jnp.concatenate([w[:, at : at + cut] for w, at in segments], 0) for segments in parts
        ]
        joined = jnp.dot(
            jnp.concatenate([jnp.concatenate(r, 1) for r in rows], 0),
            jnp.concatenate(columns, 1),
            preferred_element_type=jnp.float32,
        )
        return joined.astype(jnp.bfloat16)
    arrays = [w for segments in parts for w, _ in segments]
    layout, n = [], 0
    for segments in parts:
        layout.append(tuple((n + i, at) for i, (_, at) in enumerate(segments)))
        n += len(segments)
    vmem = pl.BlockSpec(memory_space=pltpu.VMEM)
    return pl.pallas_call(
        functools.partial(project_kernel, len(rows), halves, tuple(layout), cut),
        out_shape=jax.ShapeDtypeStruct((height, width), jnp.bfloat16),
        in_specs=[vmem] * (len(flat) + len(arrays)),
        out_specs=vmem,
        cost_estimate=pl.CostEstimate(
            flops=2 * height * width * depth,
            bytes_accessed=2 * depth * (height + width),
            transcendentals=0,
        ),
        compiler_params=pltpu.CompilerParams(vmem_limit_bytes=24 * 1024 * 1024),
        name="project",
    )(*flat, *arrays)


def settle_kernel(plan, peers, cut, turn, *refs):
    outs = refs[-peers:]
    values = []
    for groups in plan:
        blocks = []
        for kind, rows, columns in groups:
            if kind == "given":
                blocks.append(refs[rows][...])
                continue
            w = jnp.concatenate(
                [
                    jnp.concatenate([refs[n][:, at : at + cut] for n, at in segments], axis=0)
                    for segments in columns
                ],
                axis=1,
            )
            for halves in rows:
                x = jnp.concatenate([refs[n][...] for n in halves], axis=1)
                blocks.append(
                    jnp.dot(x, w, preferred_element_type=jnp.float32).astype(jnp.bfloat16)
                )
        values.append(blocks)
    for e in range(peers):
        for target in range(peers):

            @pl.when((turn[0] ^ e) == target)
            def _(e=e, target=target):
                at = 0
                for block in values[target]:
                    outs[e][at : at + block.shape[0], :] = block
                    at += block.shape[0]


def settle(turn, parts, cut, height, width):
    peers = len(parts)
    refs, plan, flops = [], [], 0

    def ref(x):
        for n, known in enumerate(refs):
            if known is x:
                return n
        refs.append(x)
        return len(refs) - 1

    for groups in parts:
        listed = []
        for group in groups:
            if group[0] == "given":
                listed.append(("given", ref(group[1]), None))
            else:
                rows = tuple(tuple(ref(x) for x in halves) for halves in group[1])
                columns = tuple(tuple((ref(w), at) for w, at in seg) for seg in group[2])
                flops += 2 * len(rows) * width * height * 512
                listed.append(("do", rows, columns))
        plan.append(tuple(listed))
    vmem = pl.BlockSpec(memory_space=pltpu.VMEM)
    return pl.pallas_call(
        functools.partial(settle_kernel, tuple(plan), peers, cut),
        out_shape=[jax.ShapeDtypeStruct((height, width), jnp.bfloat16)] * peers,
        in_specs=[pl.BlockSpec(memory_space=pltpu.SMEM)] + [vmem] * len(refs),
        out_specs=[vmem] * peers,
        cost_estimate=pl.CostEstimate(flops=flops, bytes_accessed=height * width * 8, transcendentals=0),
        compiler_params=pltpu.CompilerParams(vmem_limit_bytes=32 * 1024 * 1024),
        name="settle",
    )(turn, *refs)


def prepare_kernel(chunks, cut, info, lengths, noise, residual, gain, level, factor, *parts):
    rows, width = residual.shape
    position = info[0] + lax.broadcasted_iota(jnp.int32, (rows, 1), 0)
    shift = jnp.zeros((rows, width), jnp.float32)
    begin = jnp.int32(0)
    for d in range(lengths.shape[1]):
        end = begin + lengths[0, d] * BLK
        member = (position >= begin) & (position < end)
        shift = jnp.where(member, level[pl.ds(noise[0, d], 1), :], shift)
        begin = end
    factor[...] = gain[...] * (1.0 + shift)
    step = chunks * cut
    for j in range(chunks):
        if chunks == 1:
            parts[j][...] = residual[...]
        else:
            for b in range(width // step):
                parts[j][:, b * cut : (b + 1) * cut] = residual[
                    :, b * step + j * cut : b * step + (j + 1) * cut
                ]


def prepare(info, lengths, noise, residual, gain, level, chunks, cut):
    rows, width = residual.shape
    smem = pl.BlockSpec(memory_space=pltpu.SMEM)
    vmem = pl.BlockSpec(memory_space=pltpu.VMEM)
    out = pl.pallas_call(
        functools.partial(prepare_kernel, chunks, cut),
        out_shape=[jax.ShapeDtypeStruct((rows, width), jnp.float32)]
        + [jax.ShapeDtypeStruct((rows, width // chunks), jnp.bfloat16)] * chunks,
        in_specs=[smem, smem, smem, vmem, vmem, vmem],
        out_specs=[vmem] * (1 + chunks),
        cost_estimate=pl.CostEstimate(
            flops=8 * rows * width, bytes_accessed=8 * rows * width, transcendentals=0
        ),
        compiler_params=pltpu.CompilerParams(vmem_limit_bytes=16 * 1024 * 1024),
        name="prepare",
    )(info, lengths, noise, residual, gain[None, :], level)
    return out[0], out[1:]


def on_device(
    queries, keys, values, residual, out_weight, norm_gain, level_shift, doc_lengths, noise_level
):
    rows = queries.shape[0]
    here = lax.axis_index("srv")
    devices = lax.axis_size("srv")
    sections = lax.axis_size("section")
    peers = lax.axis_size("tp")
    mine = lax.axis_index("tp")
    whole_index = lax.axis_index("section") * devices + here
    bits = devices.bit_length() - 1
    low = 1 << LOW_BITS

    kv = jnp.concatenate([keys, values], axis=1)
    turns = -(-(devices // 2) // low)
    back = []
    for k in range(1, turns + 1):
        back.append(shifted(kv, "srv", low * k))
    beside = flipped(kv, 2)
    beside_back = flipped(jnp.stack(back), 2)
    own = here % low
    block = here - own
    order = [(k, 0) for k in range(turns + 1)] + [(k, 2) for k in range(turns + 1)]
    spots = []
    for k, x in order:
        for c in (0, 1):
            spots.append((block - low * k + (own ^ (x + c))) * rows)
    info = jnp.stack([here * rows] + spots).astype(jnp.int32)
    info = jnp.concatenate([info, doc_lengths[0].astype(jnp.int32)])
    by_head = queries.reshape(rows, -1, HEAD_SIZE).transpose(1, 0, 2)
    depth, width = out_weight.shape
    chunks = max(1, width // 128)
    cut = width // chunks
    pieces_of = []
    for j in range(chunks):
        shares = FIRST_STRETCHES if j == 0 else (1,)
        unit = depth // sum(shares)
        pieces_of.append([(sum(shares[:n]) * unit, share * unit) for n, share in enumerate(shares)])
    cuts = []
    for j in range(chunks):
        cuts.append([])
        for at, size in pieces_of[j]:
            cuts[j].append(out_weight[at : at + size, j * cut : (j + 1) * cut])
    later = [c for j in range(chunks) for n, c in enumerate(cuts[j]) if (j, n) != (0, 0)]
    beside_back, by_head, info, later = lax.optimization_barrier(
        (beside_back, by_head, info, later)
    )
    later = list(later)
    for j in range(chunks):
        for n in range(len(cuts[j])):
            if (j, n) != (0, 0):
                cuts[j][n] = later.pop(0)
    near = jnp.concatenate([jnp.stack([kv] + back + [beside]), beside_back], axis=0)
    far = flipped(near, 1)

    held = []
    for j in range(chunks):
        segments = []
        for piece in cuts[j]:
            got = {0: piece}
            for b in range(3, bits):
                got.update({r | (1 << b): flipped(w, 1 << b) for r, w in list(got.items())})
            hop = 1
            while hop < sections:
                got.update(
                    {r | (hop * devices): flipped(w, hop, "section") for r, w in list(got.items())}
                )
                hop *= 2
            segments.append(got)
        held.append(segments)
    beside_own = flipped(out_weight, 1)
    sources = []
    for j in range(chunks):
        found = {0: [(out_weight, j * cut)], 1: [(beside_own, j * cut)]}
        for got in held[j]:
            for r, w in got.items():
                if r:
                    found.setdefault(r, []).append((w, 0))
                    found.setdefault(r | 1, []).append((flipped(w, 1), 0))
        sources.append(found)

    kv_heads = keys.shape[1] // HEAD_SIZE
    groups = by_head.shape[0] // kv_heads
    attended, across = [], []
    for h in range(kv_heads):
        attended.append(
            attend(info, by_head[h * groups : (h + 1) * groups], near, far, kv_heads, h)
        )
        across.append(flipped(attended[h], 4))
    row_keys = (0, 2, 4, 6)
    beside_rows, cross_rows = [], []
    for h in range(kv_heads):
        beside_rows.append(flipped(attended[h], 2))
        cross_rows.append(flipped(across[h], 2))
    gathered = [attended, beside_rows, across, cross_rows]

    blocks = residual.shape[1] // width
    factor, residuals = prepare(
        info, doc_lengths, noise_level, residual, norm_gain, level_shift, chunks, cut
    )

    span = sections * devices // peers
    turn = whole_index // span ^ mine
    lower = sorted(r for r in sources[0] if r < span)
    returned, last = [], None
    height, broad = len(row_keys) * rows, len(lower) * cut
    for j in range(chunks):
        columns = [[sources[j][part * span + r] for r in lower] for part in range(peers)]
        early = gathered[:3] if j == 0 else gathered
        if cut % 128:
            parts = [project(gathered, columns[part], cut) for part in range(peers)]
            slots = []
            for e in range(peers):
                value = parts[0]
                for part in range(1, peers):
                    value = jnp.where((turn ^ e) == part, parts[part], value)
                slots.append(value)
        else:
            parts = []
            for part in range(peers):
                if j == 0 or part == 0:
                    parts.append([("given", project(early, columns[part], cut))])
                    if j == 0:
                        parts[part].append(("do", gathered[3:], columns[part]))
                else:
                    parts.append([("do", gathered, columns[part])])
            slots = settle(turn[None], parts, cut, height, broad)
        came = []
        for e in range(1, peers):
            came.append(flipped(slots[e], e, "tp"))
        last = came
        blocks_back = []
        for i, r in enumerate(row_keys):
            at = slice(i * rows, (i + 1) * rows)
            piece = slots[0][at].astype(jnp.float32)
            for x in came:
                piece = piece + x[at].astype(jnp.float32)
            if r:
                piece = flipped(piece.astype(jnp.bfloat16), r)
            blocks_back.append(piece)
        returned.append(blocks_back)
    hidden, squares = [], 0.0
    for j in range(chunks):
        back_here = returned[j]
        if j + 1 < chunks:
            back_here, _ = lax.optimization_barrier((back_here, last))
        pieces = {}
        for r, piece in zip(row_keys, back_here):
            piece = piece.astype(jnp.float32)
            for n, a in enumerate(lower):
                pieces[a ^ r] = piece[:, n * cut : (n + 1) * cut]
        b = 1
        while len(pieces) > 1:
            pieces = {
                r: ordered([pieces[r], pieces[r | b]], (whole_index // b) % 2)
                for r in pieces
                if not r & b
            }
            b *= 2
        hidden.append(pieces[0] + residuals[j].astype(jnp.float32))
        squares = squares + jnp.sum(hidden[j] * hidden[j], axis=1)

    hop = 1
    while hop < peers:
        squares = squares + flipped(squares, hop, "tp")
        hop *= 2
    inverse = lax.rsqrt(squares / (residual.shape[1] * peers) + 1e-06)[:, None]
    normed = jnp.concatenate(
        [hidden[j][:, b * cut : (b + 1) * cut] for b in range(blocks) for j in range(chunks)], axis=1
    )
    return (normed * inverse * factor).astype(jnp.bfloat16)


def solution(mesh):
    placed = (
        P(("section", "srv"), "tp"),
        P(("section", "srv"), "tp"),
        P(("section", "srv"), "tp"),
        P(("section", "srv"), "tp"),
        P("tp", ("section", "srv")),
        P("tp"),
        P(None, "tp"),
        P("section", None),
        P("section", None),
    )
    return jax.shard_map(
        on_device,
        mesh=mesh,
        in_specs=placed,
        out_specs=P(("section", "srv"), "tp"),
        check_vma=False,
    )
```
